256 devices in a mesh: batch: 64 (over z, y, core), group: 4 (over x).
Axes of the slice: x: 4, y: 4, z: 8, core: 2. Of those that a mesh axis runs over, the one named last changes fastest.
Arguments:
- samples_in: float32 [16384, 8192], P('batch', 'group'), may hold values from -8 to 8, as said below
- second_samples_in: float32 [16384, 8192], P('batch', 'group'), may hold values from -8 to 8, as said below
Outputs:
- standard: float32 [16384, 8192], P(None, ('group', 'batch'))
- second_standard: float32 [16384, 8192], P(None, ('group', 'batch'))
The draws below stay inside these ranges and needn't reach their ends.
Inputs may be any that keep to these rules, and one draw needn't show every extreme that they name: samples_in holds numbers from -8 to 8. second_samples_in holds numbers from -8 to 8.
All inputs are finite; a program needn't handle non-finite values.
Results may differ from the reference program's by a relative error of at most 0.0003.
Values sent between devices are 32-bit elements.
A program may use at most 64 MiB of HBM per device.

```python
import jax
import jax.numpy as jnp

ROW_DEV = 256
ROWS = 16384
COLS = 8192
N_BATCH = 64


def column_values(key, tag):
    keys = jax.random.split(jax.random.fold_in(key, tag), 4)
    level = jax.random.normal(keys[0], (1, 1, COLS), jnp.float32) * 1.0
    spread = jnp.exp(jax.random.uniform(keys[1], (1, 1, COLS), jnp.float32, -0.7, 0.7))
    drift = jax.random.normal(keys[2], (N_BATCH, 1, COLS), jnp.float32) * 1.0
    noise = jax.random.normal(keys[3], (N_BATCH, ROW_DEV, COLS), jnp.float32) * 0.6
    return level + spread * (drift + noise)


def draw_samples_in(key, part):
    values = column_values(key, 1)
    return jnp.clip(values, -8.0, 8.0).reshape(ROWS, COLS)


def draw_second_samples_in(key, part):
    values = column_values(key, 2)
    return jnp.clip(values, -8.0, 8.0).reshape(ROWS, COLS)


def setup_inputs(seed: int = 0) -> dict:
    key_list = jax.random.split(jax.random.key(seed), 3)
    return {
        "samples_in": draw_samples_in(jax.random.fold_in(key_list[2], 71), 0),
        "second_samples_in": draw_second_samples_in(jax.random.fold_in(key_list[2], 71), 0),
    }


def reference(samples_in, second_samples_in):
    wide_standard = samples_in.astype(jnp.float32)
    low_standard = jnp.mean(jnp.minimum(wide_standard, 1.0), axis=0)
    high_standard = jnp.mean(jnp.maximum(wide_standard, 1.0), axis=0)
    standard = ((wide_standard - low_standard) / (high_standard - low_standard + 0.1))
    wide_second_standard = second_samples_in.astype(jnp.float32)
    low_second_standard = jnp.mean(jnp.minimum(wide_second_standard, 1.0), axis=0)
    high_second_standard = jnp.mean(jnp.maximum(wide_second_standard, 1.0), axis=0)
    second_standard = ((wide_second_standard - low_second_standard) / (high_second_standard - low_second_standard + 0.1))
    return standard, second_standard
```

```python
import functools

import jax
import jax.numpy as jnp
from jax import lax
from jax.experimental import pallas as pl
from jax.experimental.pallas import tpu as pltpu
from jax.sharding import PartitionSpec as P

MESH = pl.DeviceIdType.MESH
NZ, NY, NC = 8, 4, 2
PLANE = NY * NC
PEERS = NZ * PLANE
HOPS = (1, 7, 2, 6, 3, 5, 4, 0)


def move_kernel(
    a_ref, b_ref, ra_ref, rb_ref, stats_ref, held, blocks, load_sems, send_sems, recv_sems
):
    rows = a_ref.shape[0]
    width = a_ref.shape[1] // PEERS
    span = width * PLANE
    total = rows * PEERS
    me = lax.axis_index("batch")
    group = lax.axis_index("group")
    z, y, c = me // PLANE, lax.rem(me // NC, NY), lax.rem(me, NC)
    sources, landed = (a_ref, b_ref), (ra_ref, rb_ref)

    barrier = pltpu.get_barrier_semaphore()

    def greet(k, carry):
        pl.semaphore_signal(
            barrier, inc=1, device_id=(lax.rem(me + k, PEERS), group), device_id_type=MESH
        )
        return carry

    def load(i, hop):
        plane = lax.rem(z + hop, NZ)
        columns = pl.ds(pl.multiple_of(plane * span, span), span)
        return pltpu.make_async_copy(
            sources[i].at[:, columns], held.at[i, :, columns], load_sems.at[i, hop]
        )

    def turn(i, hop):
        load(i, hop).wait()
        plane = lax.rem(z + hop, NZ)
        for part in range(span // 128):
            columns = pl.ds(pl.multiple_of(plane * span + part * 128, 128), 128)
            tile = held[i, :, columns].T
            per = 128 // width
            first = plane * PLANE + part * per
            for k in range(per):
                blocks[i, first + k] = tile[k * width : (k + 1) * width]

    def send(i, hop):
        plane = lax.rem(z + hop, NZ)
        for dy in range(NY):
            for dc in range(NC):
                if (hop, dy, dc) == (0, 0, 0):
                    continue
                to = plane * PLANE + lax.rem(y + dy, NY) * NC + lax.rem(c + dc, NC)
                pltpu.make_async_remote_copy(
                    src_ref=blocks.at[i, to],
                    dst_ref=landed[i].at[me],
                    send_sem=send_sems.at[i],
                    recv_sem=recv_sems.at[i, hop],
                    device_id=(to, group),
                    device_id_type=MESH,
                ).start()

    def gather(i, hop, sums):
        plane = lax.rem(z - hop + NZ, NZ)
        count = PLANE - 1 if hop == 0 else PLANE
        whole = landed[i].at[pl.ds(0, count)]
        pltpu.make_async_copy(whole, whole, recv_sems.at[i, hop]).wait()
        low, high = sums
        for k in range(PLANE):
            for part in range(rows // 128):
                x = landed[i][plane * PLANE + k, :, part * 128 : (part + 1) * 128]
                low += jnp.minimum(x, 1.0)
                high += jnp.maximum(x, 1.0)
        return low, high

    lax.fori_loop(1, PEERS, greet, 0)
    for i in range(2):
        for hop in HOPS:
            load(i, hop).start()
    for hop in HOPS:
        turn(0, hop)
    ra_ref[me] = blocks[0, me]
    pl.semaphore_wait(barrier, PEERS - 1)
    for hop in HOPS:
        send(0, hop)
    for hop in HOPS:
        turn(1, hop)
    rb_ref[me] = blocks[1, me]
    for hop in HOPS:
        send(1, hop)
    for i in range(2):
        zero = jnp.zeros((width, 128), jnp.float32)
        sums = (zero, zero)
        for hop in HOPS:
            sums = gather(i, hop, sums)
        low = jnp.sum(sums[0], axis=1, keepdims=True) * (1.0 / total)
        high = jnp.sum(sums[1], axis=1, keepdims=True) * (1.0 / total)
        stats_ref[2 * i] = jnp.broadcast_to(low, (width, 128))
        stats_ref[2 * i + 1] = jnp.broadcast_to(1.0 / (high - low + 0.1), (width, 128))
    for i in range(2):
        whole = blocks.at[i, pl.ds(0, PEERS - 1)]
        pltpu.make_async_copy(whole, whole, send_sems.at[i]).wait()


def scale_kernel(ra_ref, rb_ref, stats_ref, oa_ref, ob_ref, ready, sems):
    peers, width, rows = ra_ref.shape
    pieces = 8
    per = peers // pieces
    copies = []
    for i, (landed, out) in enumerate(((ra_ref, oa_ref), (rb_ref, ob_ref))):
        low, scale = stats_ref[2 * i], stats_ref[2 * i + 1]
        for piece in range(pieces):
            for k in range(piece * per, (piece + 1) * per):
                for part in range(0, rows, 128):
                    x = landed[k, :, part : part + 128]
                    ready[i, :, k * rows + part : k * rows + part + 128] = (x - low) * scale
            columns = pl.ds(piece * per * rows, per * rows)
            copy = pltpu.make_async_copy(
                ready.at[i, :, columns], out.at[:, columns], sems.at[i, piece]
            )
            copy.start()
            copies.append(copy)
    for copy in copies:
        copy.wait()


def shards(a, b):
    rows, width = a.shape[0], a.shape[1] // PEERS
    block = (PEERS, width, rows)
    ra, rb, stats = pl.pallas_call(
        move_kernel,
        out_shape=(
            pltpu.VMEM(block, jnp.float32),
            pltpu.VMEM(block, jnp.float32),
            pltpu.VMEM((4, width, 128), jnp.float32),
        ),
        in_specs=[pl.BlockSpec(memory_space=pltpu.HBM)] * 2,
        out_specs=[pl.BlockSpec(memory_space=pltpu.VMEM)] * 3,
        scratch_shapes=[
            pltpu.VMEM((2,) + a.shape, jnp.float32),
            pltpu.VMEM((2,) + block, jnp.float32),
            pltpu.SemaphoreType.DMA((2, NZ)),
            pltpu.SemaphoreType.DMA((2,)),
            pltpu.SemaphoreType.DMA((2, NZ)),
        ],
        compiler_params=pltpu.CompilerParams(
            collective_id=0, has_side_effects=True, vmem_limit_bytes=58 << 20
        ),
        name="move",
    )(a, b)
    wide = jax.ShapeDtypeStruct((width, PEERS * rows), jnp.float32)
    oa, ob = pl.pallas_call(
        scale_kernel,
        out_shape=(wide, wide),
        in_specs=[pl.BlockSpec(memory_space=pltpu.VMEM)] * 3,
        out_specs=[pl.BlockSpec(memory_space=pltpu.HBM)] * 2,
        scratch_shapes=[
            pltpu.VMEM((2,) + wide.shape, jnp.float32),
            pltpu.SemaphoreType.DMA((2, 8)),
        ],
        compiler_params=pltpu.CompilerParams(vmem_limit_bytes=24 << 20),
        name="scale",
    )(ra, rb, stats)
    return oa.T, ob.T


def solution(mesh):
    placed = (P("batch", "group"), P("batch", "group"))
    return jax.shard_map(
        shards,
        mesh=mesh,
        in_specs=placed,
        out_specs=(P(None, ("group", "batch")), P(None, ("group", "batch"))),
        check_vma=False,
    )
```

```python
import functools

import jax
import jax.numpy as jnp
from jax import lax
from jax.experimental import pallas as pl
from jax.experimental.pallas import tpu as pltpu
from jax.sharding import PartitionSpec as P

MESH = pl.DeviceIdType.MESH
NZ, NY, NC = 8, 4, 2
PLANE = NY * NC
PEERS = NZ * PLANE
HOPS = (1, 7, 2, 6, 3, 5, 4, 0)
OFFSETS = tuple(
    ((5 * k + 5) % NZ, (k // NZ * 3 + k) % NY, k // (NZ * NY)) for k in range(PEERS)
)
NEAR = tuple(
    (hop, dy, dc)
    for hop, dy, dc in OFFSETS
    if (hop == 0 and dy + dc > 0) or (hop in (1, 7) and dy == 0)
)
FIRST = ((1, 0, 0), (7, 0, 0), (1, 0, 1), (7, 0, 1))
SECOND = tuple((hop, dy, dc) for dy in (1, 2, 3) for dc in (0, 1) for hop in (1, 7))
THIRD = tuple(o for o in OFFSETS if o[0] not in (1, 7, 4) and o != (0, 0, 0))
LAST = tuple((0, o) for o in OFFSETS if o[0] == 4) + tuple(
    (1, o) for o in OFFSETS if o != (0, 0, 0)
)


def move_kernel(
    a_ref, b_ref, ra_ref, rb_ref, stats_ref, held, blocks, load_sems, send_sems, recv_sems, known
):
    rows = a_ref.shape[0]
    width = a_ref.shape[1] // PEERS
    span = width * PLANE
    total = rows * PEERS
    me = lax.axis_index("batch")
    group = lax.axis_index("group")
    z, y, c = me // PLANE, lax.rem(me // NC, NY), lax.rem(me, NC)
    sources, landed = (a_ref, b_ref), (ra_ref, rb_ref)

    def peer(hop, dy, dc):
        return lax.rem(z + hop, NZ) * PLANE + lax.rem(y + dy, NY) * NC + lax.rem(c + dc, NC)

    def signal(semaphore, *offset):
        pl.semaphore_signal(
            semaphore, inc=1, device_id=(peer(*offset), group), device_id_type=MESH
        )

    def load(i, hop):
        plane = lax.rem(z + hop, NZ)
        columns = pl.ds(pl.multiple_of(plane * span, span), span)
        return pltpu.make_async_copy(
            sources[i].at[:, columns], held.at[i, :, columns], load_sems.at[i, hop]
        )

    def turn(i, hop):
        load(i, hop).wait()
        plane = lax.rem(z + hop, NZ)
        for part in range(span // 128):
            columns = pl.ds(pl.multiple_of(plane * span + part * 128, 128), 128)
            tile = held[i, :, columns].T
            per = 128 // width
            first = plane * PLANE + part * per
            for k in range(per):
                blocks[i, first + k] = tile[k * width : (k + 1) * width]

    def send(i, offsets):
        for hop, dy, dc in offsets:
            to = peer(hop, dy, dc)
            pltpu.make_async_remote_copy(
                src_ref=blocks.at[i, to],
                dst_ref=landed[i].at[me],
                send_sem=send_sems.at[i],
                recv_sem=recv_sems.at[i, hop],
                device_id=(to, group),
                device_id_type=MESH,
            ).start()

    def gather(i, hop, sums):
        plane = lax.rem(z - hop + NZ, NZ)
        count = PLANE - 1 if hop == 0 else PLANE
        whole = landed[i].at[pl.ds(0, count)]
        pltpu.make_async_copy(whole, whole, recv_sems.at[i, hop]).wait()
        low, high = sums
        for k in range(PLANE):
            for part in range(rows // 128):
                x = landed[i][plane * PLANE + k, :, part * 128 : (part + 1) * 128]
                low += jnp.minimum(x, 1.0)
                high += jnp.maximum(x, 1.0)
        return low, high

    barrier = pltpu.get_barrier_semaphore()
    for offset in NEAR:
        signal(barrier, *offset)
    for i in range(2):
        for hop in HOPS:
            load(i, hop).start()
    turn(0, 1)
    turn(0, 7)
    pl.semaphore_wait(barrier, len(NEAR))
    signal(known.at[0], 1, 0, 0)
    signal(known.at[0], 7, 0, 0)
    send(0, FIRST)
    turn(0, 2)
    turn(0, 6)
    pl.semaphore_wait(known.at[0], 2)
    signal(known.at[1], 2, 0, 0)
    signal(known.at[1], 6, 0, 0)
    send(0, SECOND)
    for hop in (3, 5, 4, 0):
        turn(0, hop)
    pl.semaphore_wait(known.at[1], 2)
    signal(known.at[2], 7, 0, 0)
    send(0, THIRD)
    for hop in HOPS:
        turn(1, hop)
    ra_ref[me] = blocks[0, me]
    rb_ref[me] = blocks[1, me]
    pl.semaphore_wait(known.at[2], 1)
    for i, offset in LAST:
        send(i, (offset,))
    for i in range(2):
        zero = jnp.zeros((width, 128), jnp.float32)
        sums = (zero, zero)
        for hop in HOPS:
            sums = gather(i, hop, sums)
        low = jnp.sum(sums[0], axis=1, keepdims=True) * (1.0 / total)
        high = jnp.sum(sums[1], axis=1, keepdims=True) * (1.0 / total)
        stats_ref[2 * i] = jnp.broadcast_to(low, (width, 128))
        stats_ref[2 * i + 1] = jnp.broadcast_to(1.0 / (high - low + 0.1), (width, 128))
    for i in range(2):
        whole = blocks.at[i, pl.ds(0, PEERS - 1)]
        pltpu.make_async_copy(whole, whole, send_sems.at[i]).wait()


def scale_kernel(ra_ref, rb_ref, stats_ref, oa_ref, ob_ref, ready, sems):
    peers, width, rows = ra_ref.shape
    pieces = 8
    per = peers // pieces
    copies = []
    for i, (landed, out) in enumerate(((ra_ref, oa_ref), (rb_ref, ob_ref))):
        low, scale = stats_ref[2 * i], stats_ref[2 * i + 1]
        for piece in range(pieces):
            for k in range(piece * per, (piece + 1) * per):
                for part in range(0, rows, 128):
                    x = landed[k, :, part : part + 128]
                    ready[i, :, k * rows + part : k * rows + part + 128] = (x - low) * scale
            columns = pl.ds(piece * per * rows, per * rows)
            copy = pltpu.make_async_copy(
                ready.at[i, :, columns], out.at[:, columns], sems.at[i, piece]
            )
            copy.start()
            copies.append(copy)
    for copy in copies:
        copy.wait()


def shards(a, b):
    rows, width = a.shape[0], a.shape[1] // PEERS
    block = (PEERS, width, rows)
    ra, rb, stats = pl.pallas_call(
        move_kernel,
        out_shape=(
            pltpu.VMEM(block, jnp.float32),
            pltpu.VMEM(block, jnp.float32),
            pltpu.VMEM((4, width, 128), jnp.float32),
        ),
        in_specs=[pl.BlockSpec(memory_space=pltpu.HBM)] * 2,
        out_specs=[pl.BlockSpec(memory_space=pltpu.VMEM)] * 3,
        scratch_shapes=[
            pltpu.VMEM((2,) + a.shape, jnp.float32),
            pltpu.VMEM((2,) + block, jnp.float32),
            pltpu.SemaphoreType.DMA((2, NZ)),
            pltpu.SemaphoreType.DMA((2,)),
            pltpu.SemaphoreType.DMA((2, NZ)),
            pltpu.SemaphoreType.REGULAR((3,)),
        ],
        compiler_params=pltpu.CompilerParams(
            collective_id=0, has_side_effects=True, vmem_limit_bytes=58 << 20
        ),
        name="move",
    )(a, b)
    wide = jax.ShapeDtypeStruct((width, PEERS * rows), jnp.float32)
    oa, ob = pl.pallas_call(
        scale_kernel,
        out_shape=(wide, wide),
        in_specs=[pl.BlockSpec(memory_space=pltpu.VMEM)] * 3,
        out_specs=[pl.BlockSpec(memory_space=pltpu.HBM)] * 2,
        scratch_shapes=[
            pltpu.VMEM((2,) + wide.shape, jnp.float32),
            pltpu.SemaphoreType.DMA((2, 8)),
        ],
        compiler_params=pltpu.CompilerParams(vmem_limit_bytes=24 << 20),
        name="scale",
    )(ra, rb, stats)
    return oa.T, ob.T


def solution(mesh):
    placed = (P("batch", "group"), P("batch", "group"))
    return jax.shard_map(
        shards,
        mesh=mesh,
        in_specs=placed,
        out_specs=(P(None, ("group", "batch")), P(None, ("group", "batch"))),
        check_vma=False,
    )
```

```python
import functools

import jax
import jax.numpy as jnp
from jax import lax
from jax.experimental import pallas as pl
from jax.experimental.pallas import tpu as pltpu
from jax.sharding import PartitionSpec as P

MESH = pl.DeviceIdType.MESH
NZ, NY, NC = 8, 4, 2
PLANE = NY * NC
PEERS = NZ * PLANE
HOPS = (1, 7, 2, 6, 3, 5, 4, 0)
NEAR = tuple((0, k // NC, k % NC) for k in range(1, PLANE)) + tuple(
    (hop, 0, dc) for hop in (1, 7) for dc in range(NC)
)
FIRST = tuple((hop, 0, dc) for dc in range(NC) for hop in (1, 7))
SECOND = tuple((hop, 0, dc) for dc in range(NC) for hop in (2, 6))
SHIFTS = ((0, 0), (4, 2), (3, 3), (5, 1), (2, 0), (6, 2), (1, 1), (7, 3))
ROUNDS = tuple(
    (hop, (turn + shift) % NY, (turn + shift) // NY % NC)
    for turn in range(PLANE)
    for hop, shift in SHIFTS
)
REST = tuple(o for o in ROUNDS if o not in FIRST + SECOND + ((0, 0, 0),))


def move_kernel(
    a_ref, b_ref, ra_ref, rb_ref, stats_ref, held, blocks, load_sems, send_sems, recv_sems, known
):
    rows = a_ref.shape[0]
    width = a_ref.shape[1] // PEERS
    span = width * PLANE
    total = rows * PEERS
    me = lax.axis_index("batch")
    group = lax.axis_index("group")
    z, y, c = me // PLANE, lax.rem(me // NC, NY), lax.rem(me, NC)
    sources, landed = (a_ref, b_ref), (ra_ref, rb_ref)

    def peer(hop, dy, dc):
        across = dy + c * (NY - 2 * dy)
        return lax.rem(z + hop, NZ) * PLANE + lax.rem(y + across, NY) * NC + lax.rem(c + dc, NC)

    def signal(semaphore, *offset):
        pl.semaphore_signal(
            semaphore, inc=1, device_id=(peer(*offset), group), device_id_type=MESH
        )

    def load(i, hop):
        plane = lax.rem(z + hop, NZ)
        columns = pl.ds(pl.multiple_of(plane * span, span), span)
        return pltpu.make_async_copy(
            sources[i].at[:, columns], held.at[i, :, columns], load_sems.at[i, hop]
        )

    def turn(i, hop):
        load(i, hop).wait()
        plane = lax.rem(z + hop, NZ)
        for part in range(span // 128):
            columns = pl.ds(pl.multiple_of(plane * span + part * 128, 128), 128)
            tile = held[i, :, columns].T
            per = 128 // width
            first = plane * PLANE + part * per
            for k in range(per):
                blocks[i, first + k] = tile[k * width : (k + 1) * width]

    def send(i, offsets):
        for hop, dy, dc in offsets:
            to = peer(hop, dy, dc)
            pltpu.make_async_remote_copy(
                src_ref=blocks.at[i, to],
                dst_ref=landed[i].at[me],
                send_sem=send_sems.at[i],
                recv_sem=recv_sems.at[i, hop],
                device_id=(to, group),
                device_id_type=MESH,
            ).start()

    def gather(i, hop, sums):
        plane = lax.rem(z - hop + NZ, NZ)
        count = PLANE - 1 if hop == 0 else PLANE
        whole = landed[i].at[pl.ds(0, count)]
        pltpu.make_async_copy(whole, whole, recv_sems.at[i, hop]).wait()
        low, high = sums
        for k in range(PLANE):
            for part in range(rows // 128):
                x = landed[i][plane * PLANE + k, :, part * 128 : (part + 1) * 128]
                low += jnp.minimum(x, 1.0)
                high += jnp.maximum(x, 1.0)
        return low, high

    barrier = pltpu.get_barrier_semaphore()
    for offset in NEAR:
        signal(barrier, *offset)
    for hop in HOPS:
        for i in range(2):
            load(i, hop).start()
    turn(0, 1)
    turn(0, 7)
    pl.semaphore_wait(barrier, len(NEAR))
    signal(known.at[0], 1, 0, 0)
    signal(known.at[0], 7, 0, 0)
    send(0, FIRST)
    turn(1, 1)
    turn(1, 7)
    for i in range(2):
        turn(i, 2)
        turn(i, 6)
    send(1, FIRST)
    pl.semaphore_wait(known.at[0], 2)
    signal(known.at[1], 2, 0, 0)
    signal(known.at[1], 6, 0, 0)
    send(0, SECOND)
    send(1, SECOND)
    for i in range(2):
        for hop in (3, 5, 4, 0):
            turn(i, hop)
    pl.semaphore_wait(known.at[1], 2)
    signal(known.at[2], 7, 0, 0)
    ra_ref[me] = blocks[0, me]
    rb_ref[me] = blocks[1, me]
    pl.semaphore_wait(known.at[2], 1)
    send(0, REST)
    send(1, REST)
    for i in range(2):
        zero = jnp.zeros((width, 128), jnp.float32)
        sums = (zero, zero)
        for hop in HOPS:
            sums = gather(i, hop, sums)
        low = jnp.sum(sums[0], axis=1, keepdims=True) * (1.0 / total)
        high = jnp.sum(sums[1], axis=1, keepdims=True) * (1.0 / total)
        stats_ref[2 * i] = jnp.broadcast_to(low, (width, 128))
        stats_ref[2 * i + 1] = jnp.broadcast_to(1.0 / (high - low + 0.1), (width, 128))
    for i in range(2):
        whole = blocks.at[i, pl.ds(0, PEERS - 1)]
        pltpu.make_async_copy(whole, whole, send_sems.at[i]).wait()


def scale_kernel(ra_ref, rb_ref, stats_ref, oa_ref, ob_ref, ready, sems):
    peers, width, rows = ra_ref.shape
    pieces = 8
    per = peers // pieces
    copies = []
    for i, (landed, out) in enumerate(((ra_ref, oa_ref), (rb_ref, ob_ref))):
        low, scale = stats_ref[2 * i], stats_ref[2 * i + 1]
        for piece in range(pieces):
            for k in range(piece * per, (piece + 1) * per):
                for part in range(0, rows, 128):
                    x = landed[k, :, part : part + 128]
                    ready[i, :, k * rows + part : k * rows + part + 128] = (x - low) * scale
            columns = pl.ds(piece * per * rows, per * rows)
            copy = pltpu.make_async_copy(
                ready.at[i, :, columns], out.at[:, columns], sems.at[i, piece]
            )
            copy.start()
            copies.append(copy)
    for copy in copies:
        copy.wait()


def shards(a, b):
    rows, width = a.shape[0], a.shape[1] // PEERS
    block = (PEERS, width, rows)
    ra, rb, stats = pl.pallas_call(
        move_kernel,
        out_shape=(
            pltpu.VMEM(block, jnp.float32),
            pltpu.VMEM(block, jnp.float32),
            pltpu.VMEM((4, width, 128), jnp.float32),
        ),
        in_specs=[pl.BlockSpec(memory_space=pltpu.HBM)] * 2,
        out_specs=[pl.BlockSpec(memory_space=pltpu.VMEM)] * 3,
        scratch_shapes=[
            pltpu.VMEM((2,) + a.shape, jnp.float32),
            pltpu.VMEM((2,) + block, jnp.float32),
            pltpu.SemaphoreType.DMA((2, NZ)),
            pltpu.SemaphoreType.DMA((2,)),
            pltpu.SemaphoreType.DMA((2, NZ)),
            pltpu.SemaphoreType.REGULAR((3,)),
        ],
        compiler_params=pltpu.CompilerParams(
            collective_id=0, has_side_effects=True, vmem_limit_bytes=58 << 20
        ),
        name="move",
    )(a, b)
    wide = jax.ShapeDtypeStruct((width, PEERS * rows), jnp.float32)
    oa, ob = pl.pallas_call(
        scale_kernel,
        out_shape=(wide, wide),
        in_specs=[pl.BlockSpec(memory_space=pltpu.VMEM)] * 3,
        out_specs=[pl.BlockSpec(memory_space=pltpu.HBM)] * 2,
        scratch_shapes=[
            pltpu.VMEM((2,) + wide.shape, jnp.float32),
            pltpu.SemaphoreType.DMA((2, 8)),
        ],
        compiler_params=pltpu.CompilerParams(vmem_limit_bytes=24 << 20),
        name="scale",
    )(ra, rb, stats)
    return oa.T, ob.T


def solution(mesh):
    placed = (P("batch", "group"), P("batch", "group"))
    return jax.shard_map(
        shards,
        mesh=mesh,
        in_specs=placed,
        out_specs=(P(None, ("group", "batch")), P(None, ("group", "batch"))),
        check_vma=False,
    )
```

```python
import functools

import jax
import jax.numpy as jnp
from jax import lax
from jax.experimental import pallas as pl
from jax.experimental.pallas import tpu as pltpu
from jax.sharding import PartitionSpec as P

MESH = pl.DeviceIdType.MESH
NZ, NY, NC = 8, 4, 2
PLANE = NY * NC
PEERS = NZ * PLANE
HOPS = (1, 7, 2, 6, 3, 5, 4, 0)
LINE = ((0, 0, 1),) + tuple((hop, 0, dc) for hop in (1, 7) for dc in range(NC))
FIRST = tuple((hop, 0, dc) for dc in range(NC) for hop in (1, 7))
SECOND = tuple((hop, 0, dc) for dc in range(NC) for hop in (2, 6))
SHIFTS = ((0, 0), (4, 2), (3, 3), (5, 1), (2, 0), (6, 2), (1, 1), (7, 3))
ROUNDS = tuple(
    (hop, (turn + shift) % NY, (turn + shift) // NY % NC)
    for turn in range(PLANE)
    for hop, shift in SHIFTS
)
REST = tuple(o for o in ROUNDS if o not in FIRST + SECOND + ((0, 0, 0),))
FINAL = ((1, 1), (3, 1))
FAR = tuple(o for o in REST if o[0] == 4)
BODY = tuple(o for o in REST if o[0] != 4 and o[1:] not in FINAL)
STEP = len(BODY) // len(FAR) - 1
SPREAD = tuple(
    o for k in range(len(FAR)) for o in (FAR[k],) + BODY[k * STEP : (k + 1) * STEP]
) + BODY[len(FAR) * STEP :]


def move_kernel(
    a_ref, b_ref, ra_ref, rb_ref, stats_ref, held, blocks, load_sems, send_sems, recv_sems, known
):
    rows = a_ref.shape[0]
    width = a_ref.shape[1] // PEERS
    span = width * PLANE
    total = rows * PEERS
    me = lax.axis_index("batch")
    group = lax.axis_index("group")
    z, y, c = me // PLANE, lax.rem(me // NC, NY), lax.rem(me, NC)
    sources, landed = (a_ref, b_ref), (ra_ref, rb_ref)

    def peer(hop, dy, dc):
        across = dy + c * (NY - 2 * dy)
        return lax.rem(z + hop, NZ) * PLANE + lax.rem(y + across, NY) * NC + lax.rem(c + dc, NC)

    def signal(semaphore, *offset):
        pl.semaphore_signal(
            semaphore, inc=1, device_id=(peer(*offset), group), device_id_type=MESH
        )

    def greet(semaphore, k):
        to = z * PLANE + lax.rem(y + k + NY, NY) * NC + c
        pl.semaphore_signal(semaphore, inc=1, device_id=(to, group), device_id_type=MESH)

    def load(i, hop):
        plane = lax.rem(z + hop, NZ)
        columns = pl.ds(pl.multiple_of(plane * span, span), span)
        return pltpu.make_async_copy(
            sources[i].at[:, columns], held.at[i, :, columns], load_sems.at[i, hop]
        )

    def turn(i, hop):
        load(i, hop).wait()
        plane = lax.rem(z + hop, NZ)
        for part in range(span // 128):
            columns = pl.ds(pl.multiple_of(plane * span + part * 128, 128), 128)
            tile = held[i, :, columns].T
            per = 128 // width
            first = plane * PLANE + part * per
            for k in range(per):
                blocks[i, first + k] = tile[k * width : (k + 1) * width]

    def send(i, offsets):
        for hop, dy, dc in offsets:
            hop = lax.rem(hop + NZ, NZ)
            to = peer(hop, dy, dc)
            pltpu.make_async_remote_copy(
                src_ref=blocks.at[i, to],
                dst_ref=landed[i].at[me],
                send_sem=send_sems.at[i],
                recv_sem=recv_sems.at[i, hop],
                device_id=(to, group),
                device_id_type=MESH,
            ).start()

    def gather(i, hop, sums):
        plane = lax.rem(z - hop + NZ, NZ)
        count = PLANE - 1 if hop == 0 else PLANE
        whole = landed[i].at[pl.ds(0, count)]
        pltpu.make_async_copy(whole, whole, recv_sems.at[i, hop]).wait()
        low, high = sums
        for k in range(PLANE):
            for part in range(rows // 128):
                x = landed[i][plane * PLANE + k, :, part * 128 : (part + 1) * 128]
                low += jnp.minimum(x, 1.0)
                high += jnp.maximum(x, 1.0)
        return low, high

    barrier = pltpu.get_barrier_semaphore()
    for hop in (1, 7):
        load(0, hop).start()
    for offset in LINE:
        signal(barrier, *offset)
    for k in range(1, NY):
        pl.when(y + k < NY)(functools.partial(greet, barrier, k))
    turn(0, 1)
    turn(0, 7)
    for hop in HOPS:
        for i in range(2):
            if i > 0 or hop not in (1, 7):
                load(i, hop).start()
    pl.semaphore_wait(barrier, len(LINE) + y)
    signal(known.at[0], 1, 0, 0)
    signal(known.at[0], 7, 0, 0)
    for k in range(1, NY):
        pl.when(y >= k)(functools.partial(greet, known.at[2], -k))
    send(0, FIRST)
    turn(1, 1)
    turn(1, 7)
    for i in range(2):
        turn(i, 2)
        turn(i, 6)
    send(1, FIRST)
    pl.semaphore_wait(known.at[0], 2)
    signal(known.at[1], 2, 0, 0)
    signal(known.at[1], 6, 0, 0)
    send(0, SECOND)
    send(1, SECOND)
    for i in range(2):
        for hop in (3, 5, 4, 0):
            turn(i, hop)
    pl.semaphore_wait(known.at[1], 2)

    @pl.when(y < NY - 1)
    def _():
        pl.semaphore_wait(known.at[2], NY - 1 - y)

    for k in range(1, NY):
        greet(known.at[3], k)
    ra_ref[me] = blocks[0, me]
    rb_ref[me] = blocks[1, me]
    pl.semaphore_wait(known.at[3], NY - 1)
    send(0, REST)
    send(1, SPREAD)
    for plane in range(NZ):
        ahead = tuple((plane - z, dy, dc) for dy, dc in FINAL)
        pl.when(lax.rem(plane - z + NZ, NZ) != 4)(functools.partial(send, 1, ahead))
    for i in range(2):
        zero = jnp.zeros((width, 128), jnp.float32)
        sums = (zero, zero)
        for hop in HOPS:
            sums = gather(i, hop, sums)
        low = jnp.sum(sums[0], axis=1, keepdims=True) * (1.0 / total)
        high = jnp.sum(sums[1], axis=1, keepdims=True) * (1.0 / total)
        stats_ref[2 * i] = jnp.broadcast_to(low, (width, 128))
        stats_ref[2 * i + 1] = jnp.broadcast_to(1.0 / (high - low + 0.1), (width, 128))
    for i in range(2):
        whole = blocks.at[i, pl.ds(0, PEERS - 1)]
        pltpu.make_async_copy(whole, whole, send_sems.at[i]).wait()


def scale_kernel(ra_ref, rb_ref, stats_ref, oa_ref, ob_ref, ready, sems):
    peers, width, rows = ra_ref.shape
    pieces = 8
    per = peers // pieces
    copies = []
    for i, (landed, out) in enumerate(((ra_ref, oa_ref), (rb_ref, ob_ref))):
        low, scale = stats_ref[2 * i], stats_ref[2 * i + 1]
        for piece in range(pieces):
            for k in range(piece * per, (piece + 1) * per):
                for part in range(0, rows, 128):
                    x = landed[k, :, part : part + 128]
                    ready[i, :, k * rows + part : k * rows + part + 128] = (x - low) * scale
            columns = pl.ds(piece * per * rows, per * rows)
            copy = pltpu.make_async_copy(
                ready.at[i, :, columns], out.at[:, columns], sems.at[i, piece]
            )
            copy.start()
            copies.append(copy)
    for copy in copies:
        copy.wait()


def shards(a, b):
    rows, width = a.shape[0], a.shape[1] // PEERS
    block = (PEERS, width, rows)
    ra, rb, stats = pl.pallas_call(
        move_kernel,
        out_shape=(
            pltpu.VMEM(block, jnp.float32),
            pltpu.VMEM(block, jnp.float32),
            pltpu.VMEM((4, width, 128), jnp.float32),
        ),
        in_specs=[pl.BlockSpec(memory_space=pltpu.HBM)] * 2,
        out_specs=[pl.BlockSpec(memory_space=pltpu.VMEM)] * 3,
        scratch_shapes=[
            pltpu.VMEM((2,) + a.shape, jnp.float32),
            pltpu.VMEM((2,) + block, jnp.float32),
            pltpu.SemaphoreType.DMA((2, NZ)),
            pltpu.SemaphoreType.DMA((2,)),
            pltpu.SemaphoreType.DMA((2, NZ)),
            pltpu.SemaphoreType.REGULAR((4,)),
        ],
        compiler_params=pltpu.CompilerParams(
            collective_id=0, has_side_effects=True, vmem_limit_bytes=58 << 20
        ),
        name="move",
    )(a, b)
    wide = jax.ShapeDtypeStruct((width, PEERS * rows), jnp.float32)
    oa, ob = pl.pallas_call(
        scale_kernel,
        out_shape=(wide, wide),
        in_specs=[pl.BlockSpec(memory_space=pltpu.VMEM)] * 3,
        out_specs=[pl.BlockSpec(memory_space=pltpu.HBM)] * 2,
        scratch_shapes=[
            pltpu.VMEM((2,) + wide.shape, jnp.float32),
            pltpu.SemaphoreType.DMA((2, 8)),
        ],
        compiler_params=pltpu.CompilerParams(vmem_limit_bytes=24 << 20),
        name="scale",
    )(ra, rb, stats)
    return oa.T, ob.T


def solution(mesh):
    placed = (P("batch", "group"), P("batch", "group"))
    return jax.shard_map(
        shards,
        mesh=mesh,
        in_specs=placed,
        out_specs=(P(None, ("group", "batch")), P(None, ("group", "batch"))),
        check_vma=False,
    )
```

```python
import functools

import jax
import jax.numpy as jnp
from jax import lax
from jax.experimental import pallas as pl
from jax.experimental.pallas import tpu as pltpu
from jax.sharding import PartitionSpec as P

MESH = pl.DeviceIdType.MESH
NZ, NY, NC = 8, 4, 2
PLANE = NY * NC
PEERS = NZ * PLANE
HOPS = (1, 7, 2, 6, 3, 5, 4, 0)
LINE = ((0, 0, 1),) + tuple((hop, 0, dc) for hop in (1, 7) for dc in range(NC))
FIRST = tuple((hop, 0, dc) for dc in range(NC) for hop in (1, 7))
SECOND = tuple((hop, 0, dc) for dc in range(NC) for hop in (2, 6))
SHIFTS = ((0, 0), (4, 2), (3, 3), (5, 1), (2, 0), (6, 2), (1, 1), (7, 3))
ROUNDS = tuple(
    (hop, (turn + shift) % NY, (turn + shift) // NY % NC)
    for turn in range(PLANE)
    for hop, shift in SHIFTS
)
REST = tuple(o for o in ROUNDS if o not in FIRST + SECOND + ((0, 0, 0),))
FINAL = ((1, 1), (3, 1))
FAR = tuple(o for o in REST if o[0] == 4)
BODY = tuple(o for o in REST if o[0] != 4 and o[1:] not in FINAL)
STEP = len(BODY) // len(FAR) // 2
SPREAD = tuple(
    o for k in range(len(FAR)) for o in (FAR[k],) + BODY[k * STEP : (k + 1) * STEP]
) + BODY[len(FAR) * STEP :]


def move_kernel(
    a_ref, b_ref, ra_ref, rb_ref, stats_ref, held, blocks, load_sems, send_sems, recv_sems, known
):
    rows = a_ref.shape[0]
    width = a_ref.shape[1] // PEERS
    span = width * PLANE
    total = rows * PEERS
    me = lax.axis_index("batch")
    group = lax.axis_index("group")
    z, y, c = me // PLANE, lax.rem(me // NC, NY), lax.rem(me, NC)
    sources, landed = (a_ref, b_ref), (ra_ref, rb_ref)

    def peer(hop, dy, dc):
        across = dy + c * (NY - 2 * dy)
        return lax.rem(z + hop, NZ) * PLANE + lax.rem(y + across, NY) * NC + lax.rem(c + dc, NC)

    def signal(semaphore, *offset):
        pl.semaphore_signal(
            semaphore, inc=1, device_id=(peer(*offset), group), device_id_type=MESH
        )

    def greet(semaphore, k):
        to = z * PLANE + lax.rem(y + k + NY, NY) * NC + c
        pl.semaphore_signal(semaphore, inc=1, device_id=(to, group), device_id_type=MESH)

    def load(i, hop):
        plane = lax.rem(z + hop, NZ)
        columns = pl.ds(pl.multiple_of(plane * span, span), span)
        return pltpu.make_async_copy(
            sources[i].at[:, columns], held.at[i, :, columns], load_sems.at[i, hop]
        )

    def turn(i, hop):
        load(i, hop).wait()
        plane = lax.rem(z + hop, NZ)
        for part in range(span // 128):
            columns = pl.ds(pl.multiple_of(plane * span + part * 128, 128), 128)
            tile = held[i, :, columns].T
            per = 128 // width
            first = plane * PLANE + part * per
            for k in range(per):
                blocks[i, first + k] = tile[k * width : (k + 1) * width]

    def send(i, offsets):
        for hop, dy, dc in offsets:
            hop = lax.rem(hop + NZ, NZ)
            to = peer(hop, dy, dc)
            pltpu.make_async_remote_copy(
                src_ref=blocks.at[i, to],
                dst_ref=landed[i].at[me],
                send_sem=send_sems.at[i],
                recv_sem=recv_sems.at[i, hop],
                device_id=(to, group),
                device_id_type=MESH,
            ).start()

    def gather(i, hop, sums):
        plane = lax.rem(z - hop + NZ, NZ)
        count = PLANE - 1 if hop == 0 else PLANE
        whole = landed[i].at[pl.ds(0, count)]
        pltpu.make_async_copy(whole, whole, recv_sems.at[i, hop]).wait()
        low, high = sums
        for k in range(PLANE):
            for part in range(rows // 128):
                x = landed[i][plane * PLANE + k, :, part * 128 : (part + 1) * 128]
                low += jnp.minimum(x, 1.0)
                high += jnp.maximum(x, 1.0)
        return low, high

    barrier = pltpu.get_barrier_semaphore()
    for hop in (1, 7):
        load(0, hop).start()
    for offset in LINE:
        signal(barrier, *offset)
    for k in range(1, NY):
        pl.when(y + k < NY)(functools.partial(greet, barrier, k))
    turn(0, 1)
    turn(0, 7)
    for hop in HOPS:
        for i in range(2):
            if i > 0 or hop not in (1, 7):
                load(i, hop).start()
    pl.semaphore_wait(barrier, len(LINE) + y)
    signal(known.at[0], 1, 0, 0)
    signal(known.at[0], 7, 0, 0)
    for k in range(1, NY):
        pl.when(y >= k)(functools.partial(greet, known.at[2], -k))
    send(0, FIRST)
    turn(1, 1)
    turn(1, 7)
    for i in range(2):
        turn(i, 2)
        turn(i, 6)
    send(1, FIRST)
    pl.semaphore_wait(known.at[0], 2)
    signal(known.at[1], 2, 0, 0)
    signal(known.at[1], 6, 0, 0)
    send(0, SECOND)
    send(1, SECOND)
    for i in range(2):
        for hop in (3, 5, 4, 0):
            turn(i, hop)
    pl.semaphore_wait(known.at[1], 2)

    @pl.when(y < NY - 1)
    def _():
        pl.semaphore_wait(known.at[2], NY - 1 - y)

    for k in range(1, NY):
        greet(known.at[3], k)
    ra_ref[me] = blocks[0, me]
    rb_ref[me] = blocks[1, me]
    pl.semaphore_wait(known.at[3], NY - 1)
    send(0, REST)
    send(1, SPREAD)
    for plane in range(NZ):
        ahead = tuple((plane - z, dy, dc) for dy, dc in FINAL)
        pl.when(lax.rem(plane - z + NZ, NZ) != 4)(functools.partial(send, 1, ahead))
    for i in range(2):
        zero = jnp.zeros((width, 128), jnp.float32)
        sums = (zero, zero)
        for hop in HOPS:
            sums = gather(i, hop, sums)
        low = jnp.sum(sums[0], axis=1, keepdims=True) * (1.0 / total)
        high = jnp.sum(sums[1], axis=1, keepdims=True) * (1.0 / total)
        stats_ref[2 * i] = jnp.broadcast_to(low, (width, 128))
        stats_ref[2 * i + 1] = jnp.broadcast_to(1.0 / (high - low + 0.1), (width, 128))
    for i in range(2):
        whole = blocks.at[i, pl.ds(0, PEERS - 1)]
        pltpu.make_async_copy(whole, whole, send_sems.at[i]).wait()


def scale_kernel(ra_ref, rb_ref, stats_ref, oa_ref, ob_ref, ready, sems):
    peers, width, rows = ra_ref.shape
    pieces = 8
    per = peers // pieces
    copies = []
    for i, (landed, out) in enumerate(((ra_ref, oa_ref), (rb_ref, ob_ref))):
        low, scale = stats_ref[2 * i], stats_ref[2 * i + 1]
        for piece in range(pieces):
            for k in range(piece * per, (piece + 1) * per):
                for part in range(0, rows, 128):
                    x = landed[k, :, part : part + 128]
                    ready[i, :, k * rows + part : k * rows + part + 128] = (x - low) * scale
            columns = pl.ds(piece * per * rows, per * rows)
            copy = pltpu.make_async_copy(
                ready.at[i, :, columns], out.at[:, columns], sems.at[i, piece]
            )
            copy.start()
            copies.append(copy)
    for copy in copies:
        copy.wait()


def shards(a, b):
    rows, width = a.shape[0], a.shape[1] // PEERS
    block = (PEERS, width, rows)
    ra, rb, stats = pl.pallas_call(
        move_kernel,
        out_shape=(
            pltpu.VMEM(block, jnp.float32),
            pltpu.VMEM(block, jnp.float32),
            pltpu.VMEM((4, width, 128), jnp.float32),
        ),
        in_specs=[pl.BlockSpec(memory_space=pltpu.HBM)] * 2,
        out_specs=[pl.BlockSpec(memory_space=pltpu.VMEM)] * 3,
        scratch_shapes=[
            pltpu.VMEM((2,) + a.shape, jnp.float32),
            pltpu.VMEM((2,) + block, jnp.float32),
            pltpu.SemaphoreType.DMA((2, NZ)),
            pltpu.SemaphoreType.DMA((2,)),
            pltpu.SemaphoreType.DMA((2, NZ)),
            pltpu.SemaphoreType.REGULAR((4,)),
        ],
        compiler_params=pltpu.CompilerParams(
            collective_id=0, has_side_effects=True, vmem_limit_bytes=58 << 20
        ),
        name="move",
    )(a, b)
    wide = jax.ShapeDtypeStruct((width, PEERS * rows), jnp.float32)
    oa, ob = pl.pallas_call(
        scale_kernel,
        out_shape=(wide, wide),
        in_specs=[pl.BlockSpec(memory_space=pltpu.VMEM)] * 3,
        out_specs=[pl.BlockSpec(memory_space=pltpu.HBM)] * 2,
        scratch_shapes=[
            pltpu.VMEM((2,) + wide.shape, jnp.float32),
            pltpu.SemaphoreType.DMA((2, 8)),
        ],
        compiler_params=pltpu.CompilerParams(vmem_limit_bytes=24 << 20),
        name="scale",
    )(ra, rb, stats)
    return oa.T, ob.T


def solution(mesh):
    placed = (P("batch", "group"), P("batch", "group"))
    return jax.shard_map(
        shards,
        mesh=mesh,
        in_specs=placed,
        out_specs=(P(None, ("group", "batch")), P(None, ("group", "batch"))),
        check_vma=False,
    )
```

```python
import functools

import jax
import jax.numpy as jnp
from jax import lax
from jax.experimental import pallas as pl
from jax.experimental.pallas import tpu as pltpu
from jax.sharding import PartitionSpec as P

MESH = pl.DeviceIdType.MESH
NZ, NY, NC = 8, 4, 2
PLANE = NY * NC
PEERS = NZ * PLANE
HOPS = (1, 7, 2, 6, 3, 5, 4, 0)
LINE = ((0, 0, 1),) + tuple((hop, 0, dc) for hop in (1, 7) for dc in range(NC))
FIRST = tuple((hop, 0, dc) for dc in range(NC) for hop in (1, 7))
SECOND = tuple((hop, 0, dc) for dc in range(NC) for hop in (2, 6))
SHIFTS = ((0, 0), (4, 2), (3, 3), (5, 1), (2, 0), (6, 2), (1, 1), (7, 3))
ROUNDS = tuple(
    (hop, (turn + shift) % NY, (turn + shift) // NY % NC)
    for turn in range(PLANE)
    for hop, shift in SHIFTS
)
REST = tuple(o for o in ROUNDS if o not in FIRST + SECOND + ((0, 0, 0),))
FINAL = ((1, 1), (3, 1))
FAR = tuple(o for o in REST if o[0] == 4)
BODY = tuple(o for o in REST if o[0] != 4 and o[1:] not in FINAL)
STEP = len(BODY) // len(FAR) // 2
SPREAD = tuple(
    o for k in range(len(FAR)) for o in (FAR[k],) + BODY[k * STEP : (k + 1) * STEP]
) + BODY[len(FAR) * STEP :]


def move_kernel(
    a_ref, b_ref, ra_ref, rb_ref, stats_ref, held, blocks, load_sems, send_sems, recv_sems, known
):
    rows = a_ref.shape[0]
    width = a_ref.shape[1] // PEERS
    span = width * PLANE
    total = rows * PEERS
    me = lax.axis_index("batch")
    group = lax.axis_index("group")
    z, y, c = me // PLANE, lax.rem(me // NC, NY), lax.rem(me, NC)
    sources, landed = (a_ref, b_ref), (ra_ref, rb_ref)

    def peer(hop, dy, dc):
        across = dy + c * (NY - 2 * dy)
        return lax.rem(z + hop, NZ) * PLANE + lax.rem(y + across, NY) * NC + lax.rem(c + dc, NC)

    def signal(semaphore, *offset):
        pl.semaphore_signal(
            semaphore, inc=1, device_id=(peer(*offset), group), device_id_type=MESH
        )

    def greet(semaphore, k):
        to = z * PLANE + lax.rem(y + k + NY, NY) * NC + c
        pl.semaphore_signal(semaphore, inc=1, device_id=(to, group), device_id_type=MESH)

    def load(i, hop):
        plane = lax.rem(z + hop, NZ)
        columns = pl.ds(pl.multiple_of(plane * span, span), span)
        return pltpu.make_async_copy(
            sources[i].at[:, columns], held.at[i, :, columns], load_sems.at[i, hop]
        )

    def turn(i, hop):
        load(i, hop).wait()
        plane = lax.rem(z + hop, NZ)
        for part in range(span // 128):
            columns = pl.ds(pl.multiple_of(plane * span + part * 128, 128), 128)
            tile = held[i, :, columns].T
            per = 128 // width
            first = plane * PLANE + part * per
            for k in range(per):
                blocks[i, first + k] = tile[k * width : (k + 1) * width]

    def send(i, offsets):
        for hop, dy, dc in offsets:
            hop = lax.rem(hop + NZ, NZ)
            to = peer(hop, dy, dc)
            pltpu.make_async_remote_copy(
                src_ref=blocks.at[i, to],
                dst_ref=landed[i].at[me],
                send_sem=send_sems.at[i],
                recv_sem=recv_sems.at[i, hop],
                device_id=(to, group),
                device_id_type=MESH,
            ).start()

    def gather(i, hop, sums):
        plane = lax.rem(z - hop + NZ, NZ)
        count = PLANE - 1 if hop == 0 else PLANE
        whole = landed[i].at[pl.ds(0, count)]
        pltpu.make_async_copy(whole, whole, recv_sems.at[i, hop]).wait()
        low, high = sums
        for k in range(PLANE):
            for part in range(rows // 128):
                x = landed[i][plane * PLANE + k, :, part * 128 : (part + 1) * 128]
                low += jnp.minimum(x, 1.0)
                high += jnp.maximum(x, 1.0)
        return low, high

    barrier = pltpu.get_barrier_semaphore()
    for hop in (1, 7):
        load(0, hop).start()
    for offset in LINE:
        signal(barrier, *offset)
    for k in range(1, NY):
        pl.when(y + k < NY)(functools.partial(greet, barrier, k))
    turn(0, 1)
    turn(0, 7)
    for hop in HOPS:
        for i in range(2):
            if i > 0 or hop not in (1, 7):
                load(i, hop).start()
    pl.semaphore_wait(barrier, len(LINE) + y)
    signal(known.at[0], 1, 0, 0)
    signal(known.at[0], 7, 0, 0)
    for k in range(1, NY):
        pl.when(y >= k)(functools.partial(greet, known.at[2], -k))
    send(0, FIRST)
    turn(1, 1)
    turn(1, 7)
    for i in range(2):
        turn(i, 2)
        turn(i, 6)
    send(1, FIRST)
    pl.semaphore_wait(known.at[0], 2)
    signal(known.at[1], 2, 0, 0)
    signal(known.at[1], 6, 0, 0)
    send(0, SECOND)
    send(1, SECOND)
    for i in range(2):
        for hop in (3, 5, 4, 0):
            turn(i, hop)
    pl.semaphore_wait(known.at[1], 2)

    @pl.when(y < NY - 1)
    def _():
        pl.semaphore_wait(known.at[2], NY - 1 - y)

    for k in range(1, NY):
        greet(known.at[3], k)
    ra_ref[me] = blocks[0, me]
    rb_ref[me] = blocks[1, me]
    pl.semaphore_wait(known.at[3], NY - 1)
    send(0, REST)
    send(1, SPREAD)
    for plane in range(NZ):
        ahead = tuple((plane - z, dy, dc) for dy, dc in FINAL)
        pl.when(lax.rem(plane - z + NZ, NZ) != 4)(functools.partial(send, 1, ahead))
    for i in range(2):
        zero = jnp.zeros((width, 128), jnp.float32)
        sums = (zero, zero)
        for hop in (4, 0, 3, 5, 2, 6, 1, 7):
            sums = gather(i, hop, sums)
        low = jnp.sum(sums[0], axis=1, keepdims=True) * (1.0 / total)
        high = jnp.sum(sums[1], axis=1, keepdims=True) * (1.0 / total)
        stats_ref[2 * i] = jnp.broadcast_to(low, (width, 128))
        stats_ref[2 * i + 1] = jnp.broadcast_to(1.0 / (high - low + 0.1), (width, 128))
    for i in range(2):
        whole = blocks.at[i, pl.ds(0, PEERS - 1)]
        pltpu.make_async_copy(whole, whole, send_sems.at[i]).wait()


def scale_kernel(ra_ref, rb_ref, stats_ref, oa_ref, ob_ref, ready, sems):
    peers, width, rows = ra_ref.shape
    pieces = 8
    per = peers // pieces
    copies = []
    for i, (landed, out) in enumerate(((ra_ref, oa_ref), (rb_ref, ob_ref))):
        low, scale = stats_ref[2 * i], stats_ref[2 * i + 1]
        for piece in range(pieces):
            for k in range(piece * per, (piece + 1) * per):
                for part in range(0, rows, 128):
                    x = landed[k, :, part : part + 128]
                    ready[i, :, k * rows + part : k * rows + part + 128] = (x - low) * scale
            columns = pl.ds(piece * per * rows, per * rows)
            copy = pltpu.make_async_copy(
                ready.at[i, :, columns], out.at[:, columns], sems.at[i, piece]
            )
            copy.start()
            copies.append(copy)
    for copy in copies:
        copy.wait()


def shards(a, b):
    rows, width = a.shape[0], a.shape[1] // PEERS
    block = (PEERS, width, rows)
    ra, rb, stats = pl.pallas_call(
        move_kernel,
        out_shape=(
            pltpu.VMEM(block, jnp.float32),
            pltpu.VMEM(block, jnp.float32),
            pltpu.VMEM((4, width, 128), jnp.float32),
        ),
        in_specs=[pl.BlockSpec(memory_space=pltpu.HBM)] * 2,
        out_specs=[pl.BlockSpec(memory_space=pltpu.VMEM)] * 3,
        scratch_shapes=[
            pltpu.VMEM((2,) + a.shape, jnp.float32),
            pltpu.VMEM((2,) + block, jnp.float32),
            pltpu.SemaphoreType.DMA((2, NZ)),
            pltpu.SemaphoreType.DMA((2,)),
            pltpu.SemaphoreType.DMA((2, NZ)),
            pltpu.SemaphoreType.REGULAR((4,)),
        ],
        compiler_params=pltpu.CompilerParams(
            collective_id=0, has_side_effects=True, vmem_limit_bytes=58 << 20
        ),
        name="move",
    )(a, b)
    wide = jax.ShapeDtypeStruct((width, PEERS * rows), jnp.float32)
    oa, ob = pl.pallas_call(
        scale_kernel,
        out_shape=(wide, wide),
        in_specs=[pl.BlockSpec(memory_space=pltpu.VMEM)] * 3,
        out_specs=[pl.BlockSpec(memory_space=pltpu.HBM)] * 2,
        scratch_shapes=[
            pltpu.VMEM((2,) + wide.shape, jnp.float32),
            pltpu.SemaphoreType.DMA((2, 8)),
        ],
        compiler_params=pltpu.CompilerParams(vmem_limit_bytes=24 << 20),
        name="scale",
    )(ra, rb, stats)
    return oa.T, ob.T


def solution(mesh):
    placed = (P("batch", "group"), P("batch", "group"))
    return jax.shard_map(
        shards,
        mesh=mesh,
        in_specs=placed,
        out_specs=(P(None, ("group", "batch")), P(None, ("group", "batch"))),
        check_vma=False,
    )
```
